32 devices in a mesh: seq: 8 (over z, y), grp: 4 (over x, core).
Axes of the slice: x: 2, y: 2, z: 4, core: 2. Of those that a mesh axis runs over, the one named last changes fastest.
Arguments:
- event_codes: int32 [262144], P(('seq', 'grp')), may hold values from 0 to 255
- window_ends: int32 [24576], P(('seq', 'grp')), may hold values from 0 to 8191, as said below
- window_count: int32 [32], P(('seq', 'grp')), may hold values from 1 to 768, as said below
- handed: int32 [32], P(('seq', 'grp')), may hold values from 0 to 256, as said below
Outputs:
- window_share: float32 [16384, 256], P(('seq', 'grp'))
- share_gap: float32 [16384, 256], P(('seq', 'grp'))
The draws below stay inside these ranges and needn't reach their ends.
Inputs may be any that keep to these rules, and one draw needn't show every extreme that they name: `window_ends`: for each shard, its first window_count slots hold distinct offsets in rising order; the remaining slots hold 0. `window_count`: some shard has 768 windows in every draw. `handed`: at most the shard's window_count minus 1; 0 on the last shard of each group along grp; the windows a shard keeps plus those it receives number at most 512, and exactly 512 on some shard that passes 512 // 2 in every draw.
All inputs are finite; a program needn't handle non-finite values.
Results may differ from the reference program's by a relative error of at most 0.0003.
Values sent between devices are 32-bit elements; how exact they have to be, the bound alone decides.
No kernel may reach another device: no remote copies, remote signals or barrier semaphores. Data moves between devices by JAX's collectives and lax.ppermute only.
A program may use at most 64 MiB of HBM per device.

```python
import jax
import jax.numpy as jnp
from jax import lax

CODES = 256
WINDOW = 4096
SHARD = 8192
CAP = 512
SLOTS = 768
GROUP = 4
NSHARDS = 32
EVENTS = 262144


def window_plan(key):
    shard_ids = jnp.arange(NSHARDS, dtype=jnp.int32)
    within = shard_ids % GROUP
    handed = jax.random.randint(jax.random.fold_in(key, 101), (NSHARDS,), 0, CAP // 2 + 1)
    handed = jnp.where(within == GROUP - 1, 0, handed)
    chosen = jax.random.randint(jax.random.fold_in(key, 103), (), 0, NSHARDS // GROUP) * GROUP
    chosen = chosen + jax.random.randint(jax.random.fold_in(key, 107), (), 0, GROUP - 1)
    handed = handed.at[(chosen + NSHARDS - 1) % NSHARDS].set(0)
    handed = handed.at[chosen].set(CAP // 2)
    received = jnp.where(within == 0, 0, jnp.roll(handed, 1))
    factor_one = jax.random.randint(jax.random.fold_in(key, 109), (NSHARDS,), 0, CAP)
    factor_two = jax.random.randint(jax.random.fold_in(key, 113), (NSHARDS,), 0, CAP)
    extra = factor_one * factor_two // CAP
    loaded = jnp.minimum(received + 1 + extra, CAP)
    loaded = loaded.at[chosen].set(CAP)
    return ((loaded - received + handed).astype(jnp.int32), handed.astype(jnp.int32))


def draw_event_codes(key, part):
    relabel = jax.random.permutation(jax.random.fold_in(key, 3), CODES)
    factor_one = jax.random.randint(jax.random.fold_in(key, 5), (EVENTS,), 0, CODES)
    factor_two = jax.random.randint(jax.random.fold_in(key, 7), (EVENTS,), 0, CODES)
    skewed = factor_one * factor_two // CODES
    moving = jnp.arange(EVENTS, dtype=jnp.int32) // SHARD * CODES // (2 * NSHARDS)
    return relabel[(skewed + moving) % CODES].astype(jnp.int32)


def draw_window_ends(key, part):
    counts = window_plan(key)[0]
    shard_keys = jax.random.split(jax.random.fold_in(key, 127), NSHARDS)
    picks = jax.vmap(lambda one_key: jax.random.permutation(one_key, SHARD)[:SLOTS])(shard_keys)
    slot_ids = jnp.arange(SLOTS, dtype=jnp.int32)
    marked = jnp.where(slot_ids[None, :] < counts[:, None], picks, SHARD)
    ordered = jnp.sort(marked, axis=1)
    return jnp.where(ordered < SHARD, ordered, 0).reshape(-1).astype(jnp.int32)


def draw_window_count(key, part):
    return window_plan(key)[0]


def draw_handed(key, part):
    return window_plan(key)[1]


def setup_inputs(seed: int = 0) -> dict:
    key_list = jax.random.split(jax.random.key(seed), 5)
    event_codes = draw_event_codes(jax.random.fold_in(key_list[4], 71), 0)
    window_ends = draw_window_ends(jax.random.fold_in(key_list[4], 71), 0)
    window_count = draw_window_count(jax.random.fold_in(key_list[4], 71), 0)
    handed = draw_handed(jax.random.fold_in(key_list[4], 71), 0)
    return {"event_codes": event_codes, "window_ends": window_ends, "window_count": window_count, "handed": handed}


def reference(event_codes, window_ends, window_count, handed):
    labels = jnp.arange(CODES, dtype=jnp.int32)
    shards = event_codes.reshape(NSHARDS, SHARD)

    def shard_total(own_codes):
        return jnp.sum((own_codes[:, None] == labels[None, :]).astype(jnp.float32), axis=0)

    totals = lax.map(shard_total, shards)
    offsets = jnp.cumsum(totals, axis=0) - totals
    earlier = jnp.concatenate([jnp.full((1, SHARD), -1, jnp.int32), shards[:-1]], axis=0)
    end_rows = window_ends.reshape(NSHARDS, SLOTS)
    shard_ids = jnp.arange(NSHARDS, dtype=jnp.int32)

    def one_shard(inputs):
        own_codes, prior_codes, end_row, offset, shard_id = inputs
        joined = jnp.concatenate([prior_codes, own_codes])
        cumulative = jnp.cumsum((joined[:, None] == labels[None, :]).astype(jnp.float32), axis=0)
        upper_tally = cumulative[SHARD + end_row]
        lower_tally = cumulative[SHARD + end_row - WINDOW]
        window_tally = upper_tally - lower_tally
        running = offset[None, :] + (upper_tally - cumulative[SHARD - 1][None, :])
        end_position = shard_id * SHARD + end_row
        length = jnp.minimum(WINDOW, end_position + 1).astype(jnp.float32)
        share_rows = CODES * window_tally / length[:, None]
        gap_rows = share_rows - CODES * running / (end_position + 1).astype(jnp.float32)[:, None]
        return share_rows, gap_rows

    shares, gaps = lax.map(one_shard, (shards, earlier, end_rows, offsets, shard_ids))
    within = jnp.arange(NSHARDS, dtype=jnp.int32) % GROUP
    received = jnp.where(within == 0, 0, jnp.roll(handed, 1))
    prior_count = jnp.roll(window_count, 1)
    row_ids = jnp.arange(CAP, dtype=jnp.int32)

    def place(shard_id):
        arrived = received[shard_id]
        kept_count = window_count[shard_id] - handed[shard_id]
        prior_slot = jnp.clip(prior_count[shard_id] - arrived + row_ids, 0, SLOTS - 1)
        own_slot = jnp.clip(row_ids - arrived, 0, SLOTS - 1)
        from_prior = (row_ids < arrived)[:, None]
        own_valid = ((row_ids >= arrived) & (row_ids - arrived < kept_count))[:, None]
        previous = (shard_id + NSHARDS - 1) % NSHARDS

        def pick(table_rows):
            return jnp.where(from_prior, table_rows[previous][prior_slot],
                             jnp.where(own_valid, table_rows[shard_id][own_slot], 0.0))

        return pick(shares), pick(gaps)

    placed_share, placed_gap = lax.map(place, shard_ids)
    return placed_share.reshape(NSHARDS * CAP, CODES), placed_gap.reshape(NSHARDS * CAP, CODES)
```

```python
import jax
import jax.numpy as jnp
from jax import lax
from jax.experimental import pallas as pl
from jax.experimental.pallas import tpu as pltpu
from jax.sharding import PartitionSpec as P

CODES = 256
WINDOW = 4096
LANES = 128
BLOCK = 16
PACK = 16
AXES = ("seq", "grp")
F32 = jnp.float32
BF16 = jnp.bfloat16


def label_groups():
    base = lax.broadcasted_iota(jnp.int32, (PACK, LANES), 0).astype(F32)
    return [(base + PACK * k).astype(BF16) for k in range(CODES // PACK)]


def tally_rows(rows, labels):
    total = [None] * len(labels)
    one, zero = jnp.ones((PACK, LANES), BF16), jnp.zeros((PACK, LANES), BF16)
    for row in rows:
        wide = jnp.broadcast_to(row, (PACK, LANES)).astype(BF16)
        for k, label in enumerate(labels):
            hit = jnp.where(wide == label, one, zero)
            total[k] = hit if total[k] is None else total[k] + hit
    return total


def first_kernel(place, counts, codes, ends, out_totals, out_pack, tally):
    devices = out_totals.shape[0]
    rows = codes.shape[0]
    slots = ends.shape[1]
    values = codes[...]
    out_pack[:rows, :] = values
    held, handed = counts[0], counts[1]
    start = held - handed
    shifted = pltpu.roll(
        jnp.broadcast_to(ends[...], (8, slots)), lax.rem(slots - start, slots), axis=1
    )
    passed = (slots // 3) // LANES
    for k in range(passed):
        out_pack[rows + k : rows + k + 1, :] = shifted[:1, k * LANES : (k + 1) * LANES]
    out_pack[rows + passed : rows + passed + 1, :] = jnp.full((1, LANES), handed, jnp.int32)
    rest = out_pack.shape[0] - rows - passed - 1
    out_pack[rows + passed + 1 :, :] = jnp.zeros((rest, LANES), jnp.int32)
    wide = values.astype(F32)
    groups = tally_rows([wide[r : r + 1, :] for r in range(rows)], label_groups())
    for k, group in enumerate(groups):
        tally[k * PACK : (k + 1) * PACK, :] = group
    total = lax.dot_general(
        jnp.ones((8, LANES), BF16),
        tally[...],
        (((1,), (1,)), ((), ())),
        preferred_element_type=F32,
    )
    out_totals[...] = jnp.broadcast_to(total[:1, :].reshape(1, 1, CODES), (devices, 1, CODES))


def main_kernel(place, counts, codes, ends, pack, tail, out_share, out_base, out_weight,
                turned, side, left, mask, parts):
    shard, within = place[0], place[1]
    held, handed = counts[0], counts[1]
    rows = codes.shape[0]
    slots = ends.shape[1]
    tail_rows = tail.shape[0]
    shard_len = rows * LANES
    out_rows = out_share.shape[0]
    passed = (slots // 3) // LANES
    groups = LANES // BLOCK
    side_blocks = side.shape[0] // BLOCK
    split = LANES // tail_rows
    labels = label_groups()

    before = jnp.where(shard > 0, pack[:rows, :], -1)
    turned[...] = jnp.concatenate([before, codes[...]], axis=0).astype(F32).T
    far = jnp.where(shard > 1, tail[...], -1).astype(F32)
    step = LANES // split
    stacked = jnp.concatenate(
        [far] + [pltpu.roll(far, LANES - step * k, axis=1) for k in range(1, split)], axis=0
    )
    side[...] = stacked.T[:step, :]

    for g in range(groups):
        found = tally_rows([turned[g * BLOCK + i : g * BLOCK + i + 1, :] for i in range(BLOCK)], labels)
        for k, group in enumerate(found):
            left[k * PACK : (k + 1) * PACK, g * LANES : (g + 1) * LANES] = group
    for g in range(side_blocks):
        found = tally_rows([side[g * BLOCK + i : g * BLOCK + i + 1, :] for i in range(BLOCK)], labels)
        column = (groups + g) * LANES
        for k, group in enumerate(found):
            left[k * PACK : (k + 1) * PACK, column : column + LANES] = group
    for g in range(groups):
        here = turned[g * BLOCK : (g + 1) * BLOCK, :]
        if g + 1 < groups:
            after = turned[(g + 1) * BLOCK : (g + 2) * BLOCK, :]
        else:
            after = pltpu.roll(turned[:BLOCK, :], LANES - 1, axis=1)
        left[CODES:, g * LANES : (g + 1) * LANES] = (after - here).astype(BF16)
    lane = lax.broadcasted_iota(jnp.int32, (BLOCK, LANES), 1)
    for g in range(side_blocks):
        here = side[g * BLOCK : (g + 1) * BLOCK, :]
        if g + 1 < side_blocks:
            after = side[(g + 1) * BLOCK : (g + 2) * BLOCK, :]
        else:
            top = side[:BLOCK, :]
            after = jnp.where(
                lane < LANES - tail_rows,
                pltpu.roll(top, LANES - tail_rows, axis=1),
                pltpu.roll(top, LANES - tail_rows - 1, axis=1),
            )
            after = jnp.where(lane < LANES - 1, after, turned[:BLOCK, :1])
        column = (groups + g) * LANES
        left[CODES:, column : column + LANES] = (after - here).astype(BF16)

    got = jnp.max(pack[rows + passed : rows + passed + 1, :])
    arrived = jnp.where(within > 0, got, 0)
    own = pltpu.roll(jnp.broadcast_to(ends[...], (8, slots)), arrived, axis=1)[:1, :out_rows]
    sent = [pack[rows + k : rows + k + 1, :] for k in range(passed)]
    sent = jnp.concatenate(sent + [jnp.zeros((1, out_rows - passed * LANES), jnp.int32)], axis=1)
    row = lax.broadcasted_iota(jnp.int32, (1, out_rows), 1)
    end = jnp.where(row < arrived, sent - shard_len, own)
    valid = row < arrived + held - handed
    end = jnp.where(valid, end, 0)

    upper = end + 1 + shard_len
    lower = upper - WINDOW
    upper_block, lower_block = upper >> 4, lower >> 4
    down = lax.broadcasted_iota(jnp.int32, (PACK, out_rows), 0).astype(F32)
    downs = [(down + PACK * k).astype(BF16) for k in range(LANES // PACK)]
    one, zero = jnp.ones((PACK, out_rows), BF16), jnp.zeros((PACK, out_rows), BF16)

    def limit(value):
        bound = jnp.clip(value, 0, LANES).astype(F32)
        return jnp.broadcast_to(bound, (PACK, out_rows)).astype(BF16)

    for g in range(groups):
        high = limit((upper_block - g + groups - 1) >> 3)
        low = limit((lower_block - g + groups - 1) >> 3)
        for k in range(LANES // PACK):
            reach = jnp.where(downs[k] < high, one, zero)
            skip = jnp.where(downs[k] < low, one, zero)
            first = g * LANES + k * PACK
            mask[first : first + PACK, :out_rows] = reach - one if k * PACK < rows else reach
            mask[first : first + PACK, out_rows:] = reach - skip
    side_block = lower_block + tail_rows * groups
    for g in range(side_blocks):
        for part in range(split):
            low = limit((side_block - side_blocks * part - g + groups - 1) >> 3)
            for k in range(tail_rows // PACK):
                first = (groups + g) * LANES + part * tail_rows + k * PACK
                mask[first : first + PACK, out_rows:] = jnp.where(downs[k] < low, zero, one)

    main_depth = groups * LANES
    parts[:, :out_rows] = jnp.dot(
        left[:, :main_depth], mask[:main_depth, :out_rows], preferred_element_type=F32
    )
    parts[:, out_rows:] = jnp.dot(left[...], mask[:, out_rows:], preferred_element_type=F32)

    upper_codes = parts[CODES:, :out_rows] + turned[:BLOCK, rows : rows + 1]
    lower_codes = upper_codes - parts[CODES:, out_rows:]
    inner = lax.broadcasted_iota(jnp.int32, (BLOCK, out_rows), 0)
    upper_codes = jnp.where(inner < (upper & (BLOCK - 1)), upper_codes, -2.0)
    lower_codes = jnp.where(inner < (lower & (BLOCK - 1)), lower_codes, -2.0)
    position = (shard * shard_len + end + 1).astype(F32)
    share_weight = jnp.where(valid, CODES / jnp.minimum(position, float(WINDOW)), 0.0)
    gap_weight = jnp.where(valid, CODES / position, 0.0)
    for q in range(out_rows // LANES):
        cut = slice(q * LANES, (q + 1) * LANES)
        ups = tally_rows([upper_codes[i : i + 1, cut] for i in range(BLOCK)], labels)
        lows = tally_rows([lower_codes[i : i + 1, cut] for i in range(BLOCK)], labels)
        lower_cut = slice(out_rows + q * LANES, out_rows + (q + 1) * LANES)
        shares, bases = [], []
        for k in range(CODES // PACK):
            span = slice(k * PACK, (k + 1) * PACK)
            up = ups[k].astype(F32)
            run = parts[span, cut] + up
            tally = parts[span, lower_cut] + (up - lows[k].astype(F32))
            share = tally * share_weight[:, cut]
            shares.append(share)
            bases.append(share - run * gap_weight[:, cut])
        out_share[cut, :] = jnp.concatenate(shares, axis=0).T
        out_base[cut, :] = jnp.concatenate(bases, axis=0).T
        out_weight[cut, :] = jnp.broadcast_to(gap_weight[:, cut], (LANES, LANES)).T


def last_kernel(place, totals, base, weight, out_gap):
    devices = totals.shape[0]
    order = lax.broadcasted_iota(jnp.int32, (devices, 1, CODES), 0)
    offset = jnp.sum(jnp.where(order < place[0], totals[...], 0.0), axis=0)
    for k in range(CODES // LANES):
        cut = slice(k * LANES, (k + 1) * LANES)
        out_gap[:, cut] = base[:, cut] - weight[...] * offset[:, cut]


def local(event_codes, window_ends, window_count, handed):
    seq, grp = lax.axis_size("seq"), lax.axis_size("grp")
    devices = seq * grp
    shard_len, slots = event_codes.shape[0], window_ends.shape[0]
    rows = shard_len // LANES
    tail_rows = WINDOW // LANES
    out_rows = 2 * slots // 3
    passed = (slots // 3) // LANES
    pack_rows = -(-(rows + passed + 1) // 8) * 8
    within = lax.axis_index("grp")
    place = jnp.stack([lax.axis_index("seq") * grp + within, within]).astype(jnp.int32)
    counts = jnp.concatenate([window_count, handed])
    codes = event_codes.reshape(rows, LANES)
    ends = window_ends.reshape(1, slots)
    smem = pl.BlockSpec(memory_space=pltpu.SMEM)
    vmem = pl.BlockSpec(memory_space=pltpu.VMEM)

    totals, pack = pl.pallas_call(
        first_kernel,
        out_shape=(
            jax.ShapeDtypeStruct((devices, 1, CODES), F32),
            jax.ShapeDtypeStruct((pack_rows, LANES), jnp.int32),
        ),
        in_specs=[smem, smem, vmem, vmem],
        out_specs=(vmem, vmem),
        scratch_shapes=[pltpu.VMEM((CODES, LANES), BF16)],
        name="totals",
    )(place, counts, codes, ends)
    everyone = lax.all_to_all(totals, AXES, 0, 0, tiled=True)
    next_one = [(i, i + 1) for i in range(devices - 1)]
    next_two = [(i, i + 2) for i in range(devices - 2)]
    got_pack = lax.ppermute(pack, AXES, next_one)
    got_tail = lax.ppermute(codes[rows - tail_rows :], AXES, next_two)

    groups = LANES // BLOCK
    split = LANES // tail_rows
    depth = (rows + rows) * LANES // BLOCK + tail_rows * LANES // BLOCK
    share, base, weight = pl.pallas_call(
        main_kernel,
        out_shape=(
            jax.ShapeDtypeStruct((out_rows, CODES), F32),
            jax.ShapeDtypeStruct((out_rows, CODES), F32),
            jax.ShapeDtypeStruct((out_rows, LANES), F32),
        ),
        in_specs=[smem, smem, vmem, vmem, vmem, vmem],
        out_specs=(vmem, vmem, vmem),
        scratch_shapes=[
            pltpu.VMEM((LANES, LANES), F32),
            pltpu.VMEM((LANES // split, LANES), F32),
            pltpu.VMEM((CODES + BLOCK, depth), BF16),
            pltpu.VMEM((depth, 2 * out_rows), BF16),
            pltpu.VMEM((CODES + BLOCK, 2 * out_rows), F32),
        ],
        cost_estimate=pl.CostEstimate(
            flops=2 * (CODES + BLOCK) * depth * 2 * out_rows, bytes_accessed=2**21, transcendentals=0
        ),
        name="windows",
    )(place, counts, codes, ends, got_pack, got_tail)
    gap = pl.pallas_call(
        last_kernel,
        out_shape=jax.ShapeDtypeStruct((out_rows, CODES), F32),
        in_specs=[smem, vmem, vmem, vmem],
        out_specs=vmem,
        name="gap",
    )(place, everyone, base, weight)
    return share, gap


def solution(mesh):
    in_specs = (P(AXES), P(AXES), P(AXES), P(AXES))
    out_specs = (P(AXES, None), P(AXES, None))
    return jax.shard_map(local, mesh=mesh, in_specs=in_specs, out_specs=out_specs, check_vma=False)
```

```python
import jax
import jax.numpy as jnp
from jax import lax
from jax.experimental import pallas as pl
from jax.experimental.pallas import tpu as pltpu
from jax.sharding import PartitionSpec as P


CODES = 256
WINDOW = 4096
LANES = 128
BLOCK = 16
PACK = 16
VMEM_LIMIT = 16 * 2**20
FIRST_LIMIT = 60 * 2**20
AXES = ("seq", "grp")
F32 = jnp.float32
BF16 = jnp.bfloat16


def label_groups():
    base = lax.broadcasted_iota(jnp.int32, (PACK, LANES), 0).astype(F32)
    return [(base + PACK * k).astype(BF16) for k in range(CODES // PACK)]


def tally_rows(rows, labels):
    total = [None] * len(labels)
    one, zero = jnp.ones((PACK, LANES), BF16), jnp.zeros((PACK, LANES), BF16)
    for row in rows:
        wide = jnp.broadcast_to(row, (PACK, LANES)).astype(BF16)
        for k, label in enumerate(labels):
            hit = jnp.where(wide == label, one, zero)
            total[k] = hit if total[k] is None else total[k] + hit
    return total


def lane_row(block):
    return jnp.concatenate([block[k : k + 1, :] for k in range(block.shape[0])], axis=1)


def shard_place():
    within = lax.axis_index("grp")
    return lax.axis_index("seq") * lax.axis_size("grp") + within, within


def first_kernel(codes, ends, out_totals, out_ends, tally):
    devices = out_totals.shape[0]
    rows = codes.shape[0]
    slot_rows = ends.shape[0]
    out_ends[:slot_rows, :] = ends[...]
    used = jnp.sum((ends[...] > 0).astype(jnp.int32), axis=(0, 1), keepdims=True)
    used = used + (ends[:1, :1] == 0).astype(jnp.int32)
    out_ends[slot_rows:, :] = jnp.broadcast_to(used, (1, LANES))
    values = codes[...]
    wide = values.astype(F32)
    groups = tally_rows([wide[r : r + 1, :] for r in range(rows)], label_groups())
    for k, group in enumerate(groups):
        tally[k * PACK : (k + 1) * PACK, :] = group
    total = lax.dot_general(
        jnp.ones((8, LANES), BF16),
        tally[...],
        (((1,), (1,)), ((), ())),
        preferred_element_type=F32,
    )
    out_totals[...] = jnp.broadcast_to(total[:1, :].reshape(1, 1, CODES), (devices, 1, CODES))


def block_tallies(left, source, count, labels):
    for g in range(count):
        found = tally_rows([source[g * BLOCK + i : g * BLOCK + i + 1, :] for i in range(BLOCK)], labels)
        for k, group in enumerate(found):
            left[k * PACK : (k + 1) * PACK, g * LANES : (g + 1) * LANES] = group


def block_kernel(codes, near, out_left, out_first, turned):
    shard = shard_place()[0]
    groups = LANES // BLOCK
    before = jnp.where(shard > 0, near[...], -1)
    turned[...] = jnp.concatenate([before, codes[...]], axis=0).astype(F32).T
    block_tallies(out_left, turned, groups, label_groups())
    for g in range(groups):
        here = turned[g * BLOCK : (g + 1) * BLOCK, :]
        if g + 1 < groups:
            after = turned[(g + 1) * BLOCK : (g + 2) * BLOCK, :]
        else:
            after = pltpu.roll(turned[:BLOCK, :], LANES - 1, axis=1)
        out_left[CODES:, g * LANES : (g + 1) * LANES] = (after - here).astype(BF16)
    out_first[...] = turned[:BLOCK, :]


def main_kernel(left, first, packed, relayed, out_share, out_base, out_weight,
                side, side_left, mask, parts):
    shard, within = shard_place()
    tail_rows = WINDOW // LANES
    slot_rows = packed.shape[0] - tail_rows - 2
    slots = slot_rows * LANES
    mine, tail, meta = packed.at[tail_rows:, :], relayed.at[:tail_rows, :], relayed.at[tail_rows:, :]
    rows = left.shape[1] * BLOCK // (2 * LANES)
    shard_len = rows * LANES
    out_rows = out_share.shape[0]
    groups = LANES // BLOCK
    side_blocks = side.shape[0] // BLOCK
    split = LANES // tail_rows
    labels = label_groups()

    far = jnp.where(shard > 1, tail[...], -1).astype(F32)
    step = LANES // split
    stacked = jnp.concatenate(
        [far] + [pltpu.roll(far, LANES - step * k, axis=1) for k in range(1, split)], axis=0
    )
    side[...] = stacked.T[:step, :]
    block_tallies(side_left, side, side_blocks, labels)
    lane = lax.broadcasted_iota(jnp.int32, (BLOCK, LANES), 1)
    for g in range(side_blocks):
        here = side[g * BLOCK : (g + 1) * BLOCK, :]
        if g + 1 < side_blocks:
            after = side[(g + 1) * BLOCK : (g + 2) * BLOCK, :]
        else:
            top = side[:BLOCK, :]
            after = jnp.where(
                lane < LANES - tail_rows,
                pltpu.roll(top, LANES - tail_rows, axis=1),
                pltpu.roll(top, LANES - tail_rows - 1, axis=1),
            )
            after = jnp.where(lane < LANES - 1, after, first[:, :1])
        side_left[CODES:, g * LANES : (g + 1) * LANES] = (after - here).astype(BF16)

    handed = jnp.max(meta[slot_rows + 1 :, :])
    given = jnp.max(meta[slot_rows : slot_rows + 1, :]) - handed
    arrived = jnp.where(within > 0, handed, 0)
    kept = mine[slot_rows : slot_rows + 1, :] - mine[slot_rows + 1 :, :]
    kept = jnp.concatenate([kept] * (out_rows // LANES), axis=1)

    def rolled(block, shift):
        wide = jnp.broadcast_to(lane_row(block[:slot_rows, :]), (8, slots))
        return pltpu.roll(wide, shift, axis=1)[:1, :out_rows]

    own = rolled(mine, arrived)
    sent = rolled(meta, lax.rem(slots - given, slots))
    row = lax.broadcasted_iota(jnp.int32, (1, out_rows), 1)
    end = jnp.where(row < arrived, sent - shard_len, own)
    valid = row < arrived + kept
    end = jnp.where(valid, end, 0)

    upper = end + 1 + shard_len
    lower = upper - WINDOW
    upper_block, lower_block = upper >> 4, lower >> 4
    down = lax.broadcasted_iota(jnp.int32, (PACK, out_rows), 0).astype(F32)
    downs = [(down + PACK * k).astype(BF16) for k in range(LANES // PACK)]
    one, zero = jnp.ones((PACK, out_rows), BF16), jnp.zeros((PACK, out_rows), BF16)

    def limit(value):
        bound = jnp.clip(value, 0, LANES).astype(F32)
        return jnp.broadcast_to(bound, (PACK, out_rows)).astype(BF16)

    for g in range(groups):
        high = limit((upper_block - g + groups - 1) >> 3)
        low = limit((lower_block - g + groups - 1) >> 3)
        for k in range(LANES // PACK):
            reach = jnp.where(downs[k] < high, one, zero)
            skip = jnp.where(downs[k] < low, one, zero)
            base = g * LANES + k * PACK
            mask[base : base + PACK, :out_rows] = reach - one if k * PACK < rows else reach
            mask[base : base + PACK, out_rows:] = reach - skip
    side_block = lower_block + tail_rows * groups
    for g in range(side_blocks):
        for part in range(split):
            low = limit((side_block - side_blocks * part - g + groups - 1) >> 3)
            for k in range(tail_rows // PACK):
                base = (groups + g) * LANES + part * tail_rows + k * PACK
                mask[base : base + PACK, out_rows:] = jnp.where(downs[k] < low, zero, one)

    main_depth = groups * LANES
    parts[:, :out_rows] = jnp.dot(
        left[...], mask[:main_depth, :out_rows], preferred_element_type=F32
    )
    parts[:, out_rows:] = jnp.dot(
        left[...], mask[:main_depth, out_rows:], preferred_element_type=F32
    ) + jnp.dot(side_left[...], mask[main_depth:, out_rows:], preferred_element_type=F32)

    upper_codes = parts[CODES:, :out_rows] + first[:, rows : rows + 1]
    lower_codes = upper_codes - parts[CODES:, out_rows:]
    inner = lax.broadcasted_iota(jnp.int32, (BLOCK, out_rows), 0)
    upper_codes = jnp.where(inner < (upper & (BLOCK - 1)), upper_codes, -2.0)
    lower_codes = jnp.where(inner < (lower & (BLOCK - 1)), lower_codes, -2.0)
    position = (shard * shard_len + end + 1).astype(F32)
    share_weight = jnp.where(valid, CODES / jnp.minimum(position, float(WINDOW)), 0.0)
    gap_weight = jnp.where(valid, CODES / position, 0.0)
    for q in range(out_rows // LANES):
        cut = slice(q * LANES, (q + 1) * LANES)
        ups = tally_rows([upper_codes[i : i + 1, cut] for i in range(BLOCK)], labels)
        lows = tally_rows([lower_codes[i : i + 1, cut] for i in range(BLOCK)], labels)
        lower_cut = slice(out_rows + q * LANES, out_rows + (q + 1) * LANES)
        shares, bases = [], []
        for k in range(CODES // PACK):
            span = slice(k * PACK, (k + 1) * PACK)
            up = ups[k].astype(F32)
            run = parts[span, cut] + up
            tally = parts[span, lower_cut] + (up - lows[k].astype(F32))
            share = tally * share_weight[:, cut]
            shares.append(share)
            bases.append(share - run * gap_weight[:, cut])
        out_share[cut, :] = jnp.concatenate(shares, axis=0).T
        out_base[cut, :] = jnp.concatenate(bases, axis=0).T
        out_weight[cut, :] = jnp.broadcast_to(gap_weight[:, cut], (LANES, LANES)).T


def last_kernel(totals, base, weight, out_gap):
    devices = totals.shape[0]
    shard = shard_place()[0]
    order = lax.broadcasted_iota(jnp.int32, (devices, 1, CODES), 0)
    offset = jnp.sum(jnp.where(order < shard, totals[...], 0.0), axis=0)
    for k in range(CODES // LANES):
        cut = slice(k * LANES, (k + 1) * LANES)
        out_gap[:, cut] = base[:, cut] - weight[...] * offset[:, cut]


def local(event_codes, window_ends, window_count, handed):
    group = lax.axis_size("grp")
    devices = lax.axis_size("seq") * group
    shard_len, slots = event_codes.shape[0], window_ends.shape[0]
    rows = shard_len // LANES
    tail_rows = WINDOW // LANES
    out_rows = 2 * slots // 3
    ends = window_ends.reshape(slots // LANES, LANES)
    vmem = pl.BlockSpec(memory_space=pltpu.VMEM)
    params = pltpu.CompilerParams(vmem_limit_bytes=VMEM_LIMIT)
    to_next = [(i, (i + 1) % devices) for i in range(devices)]
    in_group = [(i, (i + 1) % group) for i in range(group)]

    near = lax.ppermute(event_codes, AXES, to_next)
    codes = event_codes.reshape(rows, LANES)
    totals, held_ends = pl.pallas_call(
        first_kernel,
        out_shape=(
            jax.ShapeDtypeStruct((devices, 1, CODES), F32),
            jax.ShapeDtypeStruct((slots // LANES + 1, LANES), jnp.int32),
        ),
        in_specs=[vmem] * 2,
        out_specs=(vmem, vmem),
        scratch_shapes=[pltpu.VMEM((CODES, LANES), BF16)],
        compiler_params=pltpu.CompilerParams(vmem_limit_bytes=FIRST_LIMIT),
        name="totals",
    )(codes, ends)
    everyone = lax.all_to_all(totals, AXES, 0, 0, tiled=True)
    near = near.reshape(rows, LANES)
    passing = jnp.broadcast_to(handed[:, None], (1, LANES))
    packed = jnp.concatenate([near[rows - tail_rows :], held_ends, passing])
    relayed = lax.ppermute(packed, "grp", in_group)

    depth = 2 * shard_len // BLOCK
    side_depth = WINDOW // BLOCK
    left, first = pl.pallas_call(
        block_kernel,
        out_shape=(
            jax.ShapeDtypeStruct((CODES + BLOCK, depth), BF16),
            jax.ShapeDtypeStruct((BLOCK, LANES), F32),
        ),
        in_specs=[vmem, vmem],
        out_specs=(vmem, vmem),
        scratch_shapes=[pltpu.VMEM((LANES, LANES), F32)],
        compiler_params=params,
        cost_estimate=pl.CostEstimate(
            flops=2 * CODES * depth * LANES, bytes_accessed=2**20, transcendentals=0
        ),
        name="blocks",
    )(codes, near)
    share, base, weight = pl.pallas_call(
        main_kernel,
        out_shape=(
            jax.ShapeDtypeStruct((out_rows, CODES), F32),
            jax.ShapeDtypeStruct((out_rows, CODES), F32),
            jax.ShapeDtypeStruct((out_rows, LANES), F32),
        ),
        in_specs=[vmem] * 4,
        out_specs=(vmem, vmem, vmem),
        scratch_shapes=[
            pltpu.VMEM((tail_rows, LANES), F32),
            pltpu.VMEM((CODES + BLOCK, side_depth), BF16),
            pltpu.VMEM((depth + side_depth, 2 * out_rows), BF16),
            pltpu.VMEM((CODES + BLOCK, 2 * out_rows), F32),
        ],
        compiler_params=params,
        cost_estimate=pl.CostEstimate(
            flops=2 * (CODES + BLOCK) * depth * 2 * out_rows,
            bytes_accessed=2**21,
            transcendentals=0,
        ),
        name="windows",
    )(left, first, packed, relayed)
    gap = pl.pallas_call(
        last_kernel,
        out_shape=jax.ShapeDtypeStruct((out_rows, CODES), F32),
        in_specs=[vmem, vmem, vmem],
        out_specs=vmem,
        compiler_params=params,
        name="gap",
    )(everyone, base, weight)
    return share, gap


def solution(mesh):
    in_specs = (P(AXES), P(AXES), P(AXES), P(AXES))
    out_specs = (P(AXES, None), P(AXES, None))
    return jax.shard_map(local, mesh=mesh, in_specs=in_specs, out_specs=out_specs, check_vma=False)
```

```python
import functools

import jax
import jax.numpy as jnp
from jax import lax
from jax.experimental import pallas as pl
from jax.experimental.pallas import tpu as pltpu
from jax.sharding import PartitionSpec as P


CODES = 256
WINDOW = 4096
LANES = 128
BLOCK = 16
PACK = 16
VMEM_LIMIT = 16 * 2**20
AXES = ("seq", "grp")
F32 = jnp.float32
BF16 = jnp.bfloat16


def label_groups():
    base = lax.broadcasted_iota(jnp.int32, (PACK, LANES), 0).astype(F32)
    return [(base + PACK * k).astype(BF16) for k in range(CODES // PACK)]


def tally_rows(rows, labels):
    total = [None] * len(labels)
    one, zero = jnp.ones((PACK, LANES), BF16), jnp.zeros((PACK, LANES), BF16)
    for row in rows:
        wide = jnp.broadcast_to(row, (PACK, LANES)).astype(BF16)
        for k, label in enumerate(labels):
            hit = jnp.where(wide == label, one, zero)
            total[k] = hit if total[k] is None else total[k] + hit
    return total


def lane_row(block):
    return jnp.concatenate([block[k : k + 1, :] for k in range(block.shape[0])], axis=1)


def shard_place():
    within = lax.axis_index("grp")
    return lax.axis_index("seq") * lax.axis_size("grp") + within, within


def first_kernel(rows, base, out_totals, tally):
    devices = out_totals.shape[0]
    values = base[:rows, :]
    wide = values.astype(F32)
    groups = tally_rows([wide[r : r + 1, :] for r in range(rows)], label_groups())
    for k, group in enumerate(groups):
        tally[k * PACK : (k + 1) * PACK, :] = group
    total = lax.dot_general(
        jnp.ones((8, LANES), BF16),
        tally[...],
        (((1,), (1,)), ((), ())),
        preferred_element_type=F32,
    )
    out_totals[...] = jnp.broadcast_to(total[:1, :].reshape(1, 1, CODES), (devices, 1, CODES))


def block_tallies(left, source, count, labels):
    for g in range(count):
        found = tally_rows([source[g * BLOCK + i : g * BLOCK + i + 1, :] for i in range(BLOCK)], labels)
        for k, group in enumerate(found):
            left[k * PACK : (k + 1) * PACK, g * LANES : (g + 1) * LANES] = group


def block_kernel(rows, base, near, out_left, out_first, out_bounds, out_count, turned):
    shard = shard_place()[0]
    groups = LANES // BLOCK
    slots = out_bounds.shape[1]

    def used(ends):
        above = jnp.sum((ends > 0).astype(jnp.int32), axis=(0, 1), keepdims=True)
        return above + (ends[:1, :1] == 0).astype(jnp.int32)

    ends, prior_ends = base[rows:, :], near[rows:, :]
    out_bounds[:1, :] = lane_row(ends)
    wide = jnp.broadcast_to(lane_row(prior_ends), (8, slots))
    out_bounds[1:, :] = pltpu.roll(wide, slots - jnp.max(used(prior_ends)), axis=1)[:1, :]
    out_count[...] = jnp.broadcast_to(used(ends), (1, LANES))
    before = jnp.where(shard > 0, near[:rows, :], -1)
    turned[...] = jnp.concatenate([before, base[:rows, :]], axis=0).astype(F32).T
    block_tallies(out_left, turned, groups, label_groups())
    for g in range(groups):
        here = turned[g * BLOCK : (g + 1) * BLOCK, :]
        if g + 1 < groups:
            after = turned[(g + 1) * BLOCK : (g + 2) * BLOCK, :]
        else:
            after = pltpu.roll(turned[:BLOCK, :], LANES - 1, axis=1)
        out_left[CODES:, g * LANES : (g + 1) * LANES] = (after - here).astype(BF16)
    out_first[...] = turned[:BLOCK, :]


def main_kernel(left, first, bounds, count, handed, relayed, out_share, out_base, out_weight,
                side, side_left, mask, parts):
    shard, within = shard_place()
    tail_rows = relayed.shape[0] - 1
    tail = relayed.at[:tail_rows, :]
    slots = bounds.shape[1]
    rows = left.shape[1] * BLOCK // (2 * LANES)
    shard_len = rows * LANES
    out_rows = out_share.shape[0]
    groups = LANES // BLOCK
    side_blocks = side.shape[0] // BLOCK
    split = LANES // tail_rows
    labels = label_groups()

    far = jnp.where(shard > 1, tail[...], -1).astype(F32)
    step = LANES // split
    stacked = jnp.concatenate(
        [far] + [pltpu.roll(far, LANES - step * k, axis=1) for k in range(1, split)], axis=0
    )
    side[...] = stacked.T[:step, :]
    block_tallies(side_left, side, side_blocks, labels)
    lane = lax.broadcasted_iota(jnp.int32, (BLOCK, LANES), 1)
    for g in range(side_blocks):
        here = side[g * BLOCK : (g + 1) * BLOCK, :]
        if g + 1 < side_blocks:
            after = side[(g + 1) * BLOCK : (g + 2) * BLOCK, :]
        else:
            top = side[:BLOCK, :]
            after = jnp.where(
                lane < LANES - tail_rows,
                pltpu.roll(top, LANES - tail_rows, axis=1),
                pltpu.roll(top, LANES - tail_rows - 1, axis=1),
            )
            after = jnp.where(lane < LANES - 1, after, first[:, :1])
        side_left[CODES:, g * LANES : (g + 1) * LANES] = (after - here).astype(BF16)

    given = jnp.max(relayed[tail_rows:, :])
    arrived = jnp.where(within > 0, given, 0)
    kept = jnp.concatenate([count[...] - handed[...]] * (out_rows // LANES), axis=1)

    def moved(row, shift):
        return pltpu.roll(jnp.broadcast_to(row, (8, slots)), shift, axis=1)[:1, :out_rows]

    own = moved(bounds[:1, :], arrived)
    sent = moved(bounds[1:, :], given)
    row = lax.broadcasted_iota(jnp.int32, (1, out_rows), 1)
    end = jnp.where(row < arrived, sent - shard_len, own)
    valid = row < arrived + kept
    end = jnp.where(valid, end, 0)

    upper = end + 1 + shard_len
    lower = upper - WINDOW
    upper_block, lower_block = upper >> 4, lower >> 4
    down = lax.broadcasted_iota(jnp.int32, (PACK, out_rows), 0).astype(F32)
    downs = [(down + PACK * k).astype(BF16) for k in range(LANES // PACK)]
    one, zero = jnp.ones((PACK, out_rows), BF16), jnp.zeros((PACK, out_rows), BF16)

    def limit(value):
        bound = jnp.clip(value, 0, LANES).astype(F32)
        return jnp.broadcast_to(bound, (PACK, out_rows)).astype(BF16)

    for g in range(groups):
        high = limit((upper_block - g + groups - 1) >> 3)
        low = limit((lower_block - g + groups - 1) >> 3)
        for k in range(LANES // PACK):
            reach = jnp.where(downs[k] < high, one, zero)
            skip = jnp.where(downs[k] < low, one, zero)
            base = g * LANES + k * PACK
            mask[base : base + PACK, :out_rows] = reach - one if k * PACK < rows else reach
            mask[base : base + PACK, out_rows:] = reach - skip
    side_block = lower_block + tail_rows * groups
    for g in range(side_blocks):
        for part in range(split):
            low = limit((side_block - side_blocks * part - g + groups - 1) >> 3)
            for k in range(tail_rows // PACK):
                base = (groups + g) * LANES + part * tail_rows + k * PACK
                mask[base : base + PACK, out_rows:] = jnp.where(downs[k] < low, zero, one)

    main_depth = groups * LANES
    parts[:, :out_rows] = jnp.dot(
        left[...], mask[:main_depth, :out_rows], preferred_element_type=F32
    )
    parts[:, out_rows:] = jnp.dot(
        left[...], mask[:main_depth, out_rows:], preferred_element_type=F32
    ) + jnp.dot(side_left[...], mask[main_depth:, out_rows:], preferred_element_type=F32)

    upper_codes = parts[CODES:, :out_rows] + first[:, rows : rows + 1]
    lower_codes = upper_codes - parts[CODES:, out_rows:]
    inner = lax.broadcasted_iota(jnp.int32, (BLOCK, out_rows), 0)
    upper_codes = jnp.where(inner < (upper & (BLOCK - 1)), upper_codes, -2.0)
    lower_codes = jnp.where(inner < (lower & (BLOCK - 1)), lower_codes, -2.0)
    position = (shard * shard_len + end + 1).astype(F32)
    share_weight = jnp.where(valid, CODES / jnp.minimum(position, float(WINDOW)), 0.0)
    gap_weight = jnp.where(valid, CODES / position, 0.0)
    for q in range(out_rows // LANES):
        cut = slice(q * LANES, (q + 1) * LANES)
        ups = tally_rows([upper_codes[i : i + 1, cut] for i in range(BLOCK)], labels)
        lows = tally_rows([lower_codes[i : i + 1, cut] for i in range(BLOCK)], labels)
        lower_cut = slice(out_rows + q * LANES, out_rows + (q + 1) * LANES)
        shares, bases = [], []
        for k in range(CODES // PACK):
            span = slice(k * PACK, (k + 1) * PACK)
            up = ups[k].astype(F32)
            run = parts[span, cut] + up
            tally = parts[span, lower_cut] + (up - lows[k].astype(F32))
            share = tally * share_weight[:, cut]
            shares.append(share)
            bases.append(share - run * gap_weight[:, cut])
        out_share[cut, :] = jnp.concatenate(shares, axis=0).T
        out_base[cut, :] = jnp.concatenate(bases, axis=0).T
        out_weight[cut, :] = jnp.broadcast_to(gap_weight[:, cut], (LANES, LANES)).T


def last_kernel(totals, share, base, weight, out_share, out_gap, gap, sent):
    devices = totals.shape[0]
    out_rows = share.shape[0]
    shared = pltpu.make_async_copy(share, out_share, sent.at[0])
    shared.start()
    shard = shard_place()[0]
    order = lax.broadcasted_iota(jnp.int32, (devices, 1, CODES), 0)
    offset = jnp.sum(jnp.where(order < shard, totals[...], 0.0), axis=0)
    pieces = out_rows // LANES
    copies = []
    for p in range(pieces):
        span = pl.ds(p * LANES, LANES)
        for k in range(CODES // LANES):
            cut = slice(k * LANES, (k + 1) * LANES)
            gap[span, cut] = base[span, cut] - weight[span, :] * offset[:, cut]
        copies.append(pltpu.make_async_copy(gap.at[span], out_gap.at[span], sent.at[1 + p]))
        copies[-1].start()
    shared.wait()
    for copy in copies:
        copy.wait()


def local(event_codes, window_ends, window_count, handed):
    group = lax.axis_size("grp")
    devices = lax.axis_size("seq") * group
    shard_len, slots = event_codes.shape[0], window_ends.shape[0]
    rows = shard_len // LANES
    tail_rows = WINDOW // LANES
    out_rows = 2 * slots // 3
    hbm = pl.BlockSpec(memory_space=pltpu.HBM)
    vmem = pl.BlockSpec(memory_space=pltpu.VMEM)
    params = pltpu.CompilerParams(vmem_limit_bytes=VMEM_LIMIT)
    to_next = [(i, (i + 1) % devices) for i in range(devices)]
    in_group = [(i, (i + 1) % group) for i in range(group)]

    base = jnp.concatenate(
        [event_codes.reshape(rows, LANES), window_ends.reshape(slots // LANES, LANES)]
    )
    near = lax.ppermute(base, AXES, to_next)
    totals = pl.pallas_call(
        functools.partial(first_kernel, rows),
        out_shape=jax.ShapeDtypeStruct((devices, 1, CODES), F32),
        in_specs=[vmem],
        out_specs=vmem,
        scratch_shapes=[pltpu.VMEM((CODES, LANES), BF16)],
        compiler_params=params,
        name="totals",
    )(base)
    everyone = lax.all_to_all(totals, AXES, 0, 0, tiled=True)
    passing = jnp.broadcast_to(handed[:, None], (1, LANES))
    packed = jnp.concatenate([near[rows - tail_rows : rows], passing])
    relayed = lax.ppermute(packed, "grp", in_group)

    depth = 2 * shard_len // BLOCK
    side_depth = WINDOW // BLOCK
    left, first, bounds, count = pl.pallas_call(
        functools.partial(block_kernel, rows),
        out_shape=(
            jax.ShapeDtypeStruct((CODES + BLOCK, depth), BF16),
            jax.ShapeDtypeStruct((BLOCK, LANES), F32),
            jax.ShapeDtypeStruct((2, slots), jnp.int32),
            jax.ShapeDtypeStruct((1, LANES), jnp.int32),
        ),
        in_specs=[vmem, vmem],
        out_specs=(vmem, vmem, vmem, vmem),
        scratch_shapes=[pltpu.VMEM((LANES, LANES), F32)],
        compiler_params=params,
        cost_estimate=pl.CostEstimate(
            flops=2 * CODES * depth * LANES, bytes_accessed=2**20, transcendentals=0
        ),
        name="blocks",
    )(base, near)
    share, rest, weight = pl.pallas_call(
        main_kernel,
        out_shape=(
            jax.ShapeDtypeStruct((out_rows, CODES), F32),
            jax.ShapeDtypeStruct((out_rows, CODES), F32),
            jax.ShapeDtypeStruct((out_rows, LANES), F32),
        ),
        in_specs=[vmem] * 6,
        out_specs=(vmem, vmem, vmem),
        scratch_shapes=[
            pltpu.VMEM((tail_rows, LANES), F32),
            pltpu.VMEM((CODES + BLOCK, side_depth), BF16),
            pltpu.VMEM((depth + side_depth, 2 * out_rows), BF16),
            pltpu.VMEM((CODES + BLOCK, 2 * out_rows), F32),
        ],
        compiler_params=params,
        cost_estimate=pl.CostEstimate(
            flops=2 * (CODES + BLOCK) * depth * 2 * out_rows,
            bytes_accessed=2**21,
            transcendentals=0,
        ),
        name="windows",
    )(left, first, bounds, count, passing, relayed)
    share, gap = pl.pallas_call(
        last_kernel,
        out_shape=(
            jax.ShapeDtypeStruct((out_rows, CODES), F32),
            jax.ShapeDtypeStruct((out_rows, CODES), F32),
        ),
        in_specs=[vmem] * 4,
        out_specs=(hbm, hbm),
        scratch_shapes=[
            pltpu.VMEM((out_rows, CODES), F32),
            pltpu.SemaphoreType.DMA((1 + out_rows // LANES,)),
        ],
        compiler_params=params,
        name="gap",
    )(everyone, share, rest, weight)
    return share, gap


def solution(mesh):
    in_specs = (P(AXES), P(AXES), P(AXES), P(AXES))
    out_specs = (P(AXES, None), P(AXES, None))
    return jax.shard_map(local, mesh=mesh, in_specs=in_specs, out_specs=out_specs, check_vma=False)
```

```python
import functools

import jax
import jax.numpy as jnp
from jax import lax
from jax.experimental import pallas as pl
from jax.experimental.pallas import tpu as pltpu
from jax.sharding import PartitionSpec as P


CODES = 256
WINDOW = 4096
LANES = 128
BLOCK = 16
PACK = 16
VMEM_LIMIT = 16 * 2**20
AXES = ("seq", "grp")
F32 = jnp.float32
BF16 = jnp.bfloat16


def label_groups():
    base = lax.broadcasted_iota(jnp.int32, (PACK, LANES), 0).astype(F32)
    return [(base + PACK * k).astype(BF16) for k in range(CODES // PACK)]


def tally_rows(rows, labels):
    total = [None] * len(labels)
    one, zero = jnp.ones((PACK, LANES), BF16), jnp.zeros((PACK, LANES), BF16)
    for row in rows:
        wide = jnp.broadcast_to(row, (PACK, LANES)).astype(BF16)
        for k, label in enumerate(labels):
            hit = jnp.where(wide == label, one, zero)
            total[k] = hit if total[k] is None else total[k] + hit
    return total


def lane_row(block):
    return jnp.concatenate([block[k : k + 1, :] for k in range(block.shape[0])], axis=1)


def shard_place():
    within = lax.axis_index("grp")
    return lax.axis_index("seq") * lax.axis_size("grp") + within, within


def first_kernel(rows, base, out_totals):
    devices = out_totals.shape[0]
    values = base[:rows, :]
    half = CODES // PACK
    labels = lax.broadcasted_iota(jnp.int32, (PACK, LANES), 0).astype(F32).astype(BF16)
    one, zero = jnp.ones((PACK, LANES), BF16), jnp.zeros((PACK, LANES), BF16)
    highs, lows = [], []
    for part, hits in (((values >> 4).astype(F32), highs), ((values & (half - 1)).astype(F32), lows)):
        for r in range(rows):
            wide = jnp.broadcast_to(part[r : r + 1, :], (PACK, LANES)).astype(BF16)
            hits.append(jnp.where(wide == labels, one, zero))
    pair = lax.dot_general(
        jnp.concatenate(highs, axis=1),
        jnp.concatenate(lows, axis=1),
        (((1,), (1,)), ((), ())),
        preferred_element_type=F32,
    )
    spread = jnp.concatenate([pair, jnp.zeros((PACK, LANES - half), F32)], axis=1)
    lines = []
    for k in range(CODES // LANES):
        step = LANES // half
        turn = pltpu.roll(spread[k * step : (k + 1) * step, :], 0, axis=1, stride=half, stride_axis=0)
        lines.append(jnp.sum(turn, axis=0, keepdims=True))
    total = jnp.concatenate(lines, axis=1)
    out_totals[...] = jnp.broadcast_to(total.reshape(1, 1, CODES), (devices, 1, CODES))


def block_tallies(left, source, count, labels):
    for g in range(count):
        found = tally_rows([source[g * BLOCK + i : g * BLOCK + i + 1, :] for i in range(BLOCK)], labels)
        for k, group in enumerate(found):
            left[k * PACK : (k + 1) * PACK, g * LANES : (g + 1) * LANES] = group


def block_kernel(rows, base, near, out_left, out_first, out_bounds, out_count, turned):
    shard = shard_place()[0]
    groups = LANES // BLOCK
    slots = out_bounds.shape[1]

    def used(ends):
        above = jnp.sum((ends > 0).astype(jnp.int32), axis=(0, 1), keepdims=True)
        return above + (ends[:1, :1] == 0).astype(jnp.int32)

    ends, prior_ends = base[rows:, :], near[rows:, :]
    out_bounds[:1, :] = lane_row(ends)
    wide = jnp.broadcast_to(lane_row(prior_ends), (8, slots))
    out_bounds[1:, :] = pltpu.roll(wide, slots - jnp.max(used(prior_ends)), axis=1)[:1, :]
    out_count[...] = jnp.broadcast_to(used(ends), (1, LANES))
    before = jnp.where(shard > 0, near[:rows, :], -1)
    turned[...] = jnp.concatenate([before, base[:rows, :]], axis=0).astype(F32).T
    block_tallies(out_left, turned, groups, label_groups())
    for g in range(groups):
        here = turned[g * BLOCK : (g + 1) * BLOCK, :]
        if g + 1 < groups:
            after = turned[(g + 1) * BLOCK : (g + 2) * BLOCK, :]
        else:
            after = pltpu.roll(turned[:BLOCK, :], LANES - 1, axis=1)
        out_left[CODES:, g * LANES : (g + 1) * LANES] = (after - here).astype(BF16)
    out_first[...] = turned[:BLOCK, :]


def main_kernel(left, first, bounds, count, handed, relayed, out_share, out_base, out_weight,
                side, side_left, mask, parts, share_rows, leave):
    shard, within = shard_place()
    tail_rows = relayed.shape[0] - 1
    tail = relayed.at[:tail_rows, :]
    slots = bounds.shape[1]
    rows = left.shape[1] * BLOCK // (2 * LANES)
    shard_len = rows * LANES
    out_rows = out_base.shape[0]
    groups = LANES // BLOCK
    side_blocks = side.shape[0] // BLOCK
    split = LANES // tail_rows
    labels = label_groups()

    far = jnp.where(shard > 1, tail[...], -1).astype(F32)
    step = LANES // split
    stacked = jnp.concatenate(
        [far] + [pltpu.roll(far, LANES - step * k, axis=1) for k in range(1, split)], axis=0
    )
    side[...] = stacked.T[:step, :]
    block_tallies(side_left, side, side_blocks, labels)
    lane = lax.broadcasted_iota(jnp.int32, (BLOCK, LANES), 1)
    for g in range(side_blocks):
        here = side[g * BLOCK : (g + 1) * BLOCK, :]
        if g + 1 < side_blocks:
            after = side[(g + 1) * BLOCK : (g + 2) * BLOCK, :]
        else:
            top = side[:BLOCK, :]
            after = jnp.where(
                lane < LANES - tail_rows,
                pltpu.roll(top, LANES - tail_rows, axis=1),
                pltpu.roll(top, LANES - tail_rows - 1, axis=1),
            )
            after = jnp.where(lane < LANES - 1, after, first[:, :1])
        side_left[CODES:, g * LANES : (g + 1) * LANES] = (after - here).astype(BF16)

    given = jnp.max(relayed[tail_rows:, :])
    arrived = jnp.where(within > 0, given, 0)
    kept = jnp.concatenate([count[...] - handed[...]] * (out_rows // LANES), axis=1)

    def moved(row, shift):
        return pltpu.roll(jnp.broadcast_to(row, (8, slots)), shift, axis=1)[:1, :out_rows]

    own = moved(bounds[:1, :], arrived)
    sent = moved(bounds[1:, :], given)
    row = lax.broadcasted_iota(jnp.int32, (1, out_rows), 1)
    end = jnp.where(row < arrived, sent - shard_len, own)
    valid = row < arrived + kept
    end = jnp.where(valid, end, 0)

    upper = end + 1 + shard_len
    lower = upper - WINDOW
    upper_block, lower_block = upper >> 4, lower >> 4
    down = lax.broadcasted_iota(jnp.int32, (PACK, out_rows), 0).astype(F32)
    downs = [(down + PACK * k).astype(BF16) for k in range(LANES // PACK)]
    one, zero = jnp.ones((PACK, out_rows), BF16), jnp.zeros((PACK, out_rows), BF16)

    def limit(value):
        bound = jnp.clip(value, 0, LANES).astype(F32)
        return jnp.broadcast_to(bound, (PACK, out_rows)).astype(BF16)

    for g in range(groups):
        high = limit((upper_block - g + groups - 1) >> 3)
        low = limit((lower_block - g + groups - 1) >> 3)
        for k in range(LANES // PACK):
            reach = jnp.where(downs[k] < high, one, zero)
            skip = jnp.where(downs[k] < low, one, zero)
            base = g * LANES + k * PACK
            mask[base : base + PACK, :out_rows] = reach - one if k * PACK < rows else reach
            mask[base : base + PACK, out_rows:] = reach - skip
    side_block = lower_block + tail_rows * groups
    for g in range(side_blocks):
        for part in range(split):
            low = limit((side_block - side_blocks * part - g + groups - 1) >> 3)
            for k in range(tail_rows // PACK):
                base = (groups + g) * LANES + part * tail_rows + k * PACK
                mask[base : base + PACK, out_rows:] = jnp.where(downs[k] < low, zero, one)

    main_depth = groups * LANES
    parts[:, :out_rows] = jnp.dot(
        left[...], mask[:main_depth, :out_rows], preferred_element_type=F32
    )
    parts[:, out_rows:] = jnp.dot(
        left[...], mask[:main_depth, out_rows:], preferred_element_type=F32
    ) + jnp.dot(side_left[...], mask[main_depth:, out_rows:], preferred_element_type=F32)

    upper_codes = parts[CODES:, :out_rows] + first[:, rows : rows + 1]
    lower_codes = upper_codes - parts[CODES:, out_rows:]
    inner = lax.broadcasted_iota(jnp.int32, (BLOCK, out_rows), 0)
    upper_codes = jnp.where(inner < (upper & (BLOCK - 1)), upper_codes, -2.0)
    lower_codes = jnp.where(inner < (lower & (BLOCK - 1)), lower_codes, -2.0)
    position = (shard * shard_len + end + 1).astype(F32)
    share_weight = jnp.where(valid, CODES / jnp.minimum(position, float(WINDOW)), 0.0)
    gap_weight = jnp.where(valid, CODES / position, 0.0)
    copies = []
    for q in range(out_rows // LANES):
        cut = slice(q * LANES, (q + 1) * LANES)
        ups = tally_rows([upper_codes[i : i + 1, cut] for i in range(BLOCK)], labels)
        lows = tally_rows([lower_codes[i : i + 1, cut] for i in range(BLOCK)], labels)
        lower_cut = slice(out_rows + q * LANES, out_rows + (q + 1) * LANES)
        shares, bases = [], []
        for k in range(CODES // PACK):
            span = slice(k * PACK, (k + 1) * PACK)
            up = ups[k].astype(F32)
            run = parts[span, cut] + up
            tally = parts[span, lower_cut] + (up - lows[k].astype(F32))
            share = tally * share_weight[:, cut]
            shares.append(share)
            bases.append(share - run * gap_weight[:, cut])
        share_rows[cut, :] = jnp.concatenate(shares, axis=0).T
        copies.append(pltpu.make_async_copy(share_rows.at[cut], out_share.at[cut], leave.at[q]))
        copies[-1].start()
        out_base[cut, :] = jnp.concatenate(bases, axis=0).T
        out_weight[cut, :] = jnp.broadcast_to(gap_weight[:, cut], (LANES, LANES)).T
    for copy in copies:
        copy.wait()


def last_kernel(totals, base, weight, out_gap, gap, sent):
    devices = totals.shape[0]
    out_rows = base.shape[0]
    shard = shard_place()[0]
    order = lax.broadcasted_iota(jnp.int32, (devices, 1, CODES), 0)
    offset = jnp.sum(jnp.where(order < shard, totals[...], 0.0), axis=0)
    pieces = out_rows // LANES
    copies = []
    for p in range(pieces):
        span = pl.ds(p * LANES, LANES)
        for k in range(CODES // LANES):
            cut = slice(k * LANES, (k + 1) * LANES)
            gap[span, cut] = base[span, cut] - weight[span, :] * offset[:, cut]
        copies.append(pltpu.make_async_copy(gap.at[span], out_gap.at[span], sent.at[p]))
        copies[-1].start()
    for copy in copies:
        copy.wait()


def local(event_codes, window_ends, window_count, handed):
    group = lax.axis_size("grp")
    devices = lax.axis_size("seq") * group
    shard_len, slots = event_codes.shape[0], window_ends.shape[0]
    rows = shard_len // LANES
    tail_rows = WINDOW // LANES
    out_rows = 2 * slots // 3
    hbm = pl.BlockSpec(memory_space=pltpu.HBM)
    vmem = pl.BlockSpec(memory_space=pltpu.VMEM)
    params = pltpu.CompilerParams(vmem_limit_bytes=VMEM_LIMIT)
    to_next = [(i, (i + 1) % devices) for i in range(devices)]
    in_group = [(i, (i + 1) % group) for i in range(group)]

    base = jnp.concatenate(
        [event_codes.reshape(rows, LANES), window_ends.reshape(slots // LANES, LANES)]
    )
    near = lax.ppermute(base, AXES, to_next)
    totals = pl.pallas_call(
        functools.partial(first_kernel, rows),
        out_shape=jax.ShapeDtypeStruct((devices, 1, CODES), F32),
        in_specs=[vmem],
        out_specs=vmem,
        compiler_params=params,
        name="totals",
    )(base)
    everyone = lax.all_to_all(totals, AXES, 0, 0, tiled=True)
    passing = jnp.broadcast_to(handed[:, None], (1, LANES))
    packed = jnp.concatenate([near[rows - tail_rows : rows], passing])
    relayed = lax.ppermute(packed, "grp", in_group)

    depth = 2 * shard_len // BLOCK
    side_depth = WINDOW // BLOCK
    left, first, bounds, count = pl.pallas_call(
        functools.partial(block_kernel, rows),
        out_shape=(
            jax.ShapeDtypeStruct((CODES + BLOCK, depth), BF16),
            jax.ShapeDtypeStruct((BLOCK, LANES), F32),
            jax.ShapeDtypeStruct((2, slots), jnp.int32),
            jax.ShapeDtypeStruct((1, LANES), jnp.int32),
        ),
        in_specs=[vmem, vmem],
        out_specs=(vmem, vmem, vmem, vmem),
        scratch_shapes=[pltpu.VMEM((LANES, LANES), F32)],
        compiler_params=params,
        cost_estimate=pl.CostEstimate(
            flops=2 * CODES * depth * LANES, bytes_accessed=2**20, transcendentals=0
        ),
        name="blocks",
    )(base, near)
    share, rest, weight = pl.pallas_call(
        main_kernel,
        out_shape=(
            jax.ShapeDtypeStruct((out_rows, CODES), F32),
            jax.ShapeDtypeStruct((out_rows, CODES), F32),
            jax.ShapeDtypeStruct((out_rows, LANES), F32),
        ),
        in_specs=[vmem] * 6,
        out_specs=(hbm, vmem, vmem),
        scratch_shapes=[
            pltpu.VMEM((tail_rows, LANES), F32),
            pltpu.VMEM((CODES + BLOCK, side_depth), BF16),
            pltpu.VMEM((depth + side_depth, 2 * out_rows), BF16),
            pltpu.VMEM((CODES + BLOCK, 2 * out_rows), F32),
            pltpu.VMEM((out_rows, CODES), F32),
            pltpu.SemaphoreType.DMA((out_rows // LANES,)),
        ],
        compiler_params=params,
        cost_estimate=pl.CostEstimate(
            flops=2 * (CODES + BLOCK) * depth * 2 * out_rows,
            bytes_accessed=2**21,
            transcendentals=0,
        ),
        name="windows",
    )(left, first, bounds, count, passing, relayed)
    gap = pl.pallas_call(
        last_kernel,
        out_shape=jax.ShapeDtypeStruct((out_rows, CODES), F32),
        in_specs=[vmem] * 3,
        out_specs=hbm,
        scratch_shapes=[
            pltpu.VMEM((out_rows, CODES), F32),
            pltpu.SemaphoreType.DMA((out_rows // LANES,)),
        ],
        compiler_params=params,
        name="gap",
    )(everyone, rest, weight)
    return share, gap


def solution(mesh):
    in_specs = (P(AXES), P(AXES), P(AXES), P(AXES))
    out_specs = (P(AXES, None), P(AXES, None))
    return jax.shard_map(local, mesh=mesh, in_specs=in_specs, out_specs=out_specs, check_vma=False)
```

```python
import functools

import jax
import jax.numpy as jnp
from jax import lax
from jax.experimental import pallas as pl
from jax.experimental.pallas import tpu as pltpu
from jax.sharding import PartitionSpec as P


CODES = 256
WINDOW = 4096
LANES = 128
BLOCK = 16
PACK = 16
VMEM_LIMIT = 16 * 2**20
AXES = ("seq", "grp")
F32 = jnp.float32
BF16 = jnp.bfloat16


def label_groups():
    base = lax.broadcasted_iota(jnp.int32, (PACK, LANES), 0).astype(F32)
    return [(base + PACK * k).astype(BF16) for k in range(CODES // PACK)]


def tally_rows(rows, labels):
    total = [None] * len(labels)
    one, zero = jnp.ones((PACK, LANES), BF16), jnp.zeros((PACK, LANES), BF16)
    for row in rows:
        wide = jnp.broadcast_to(row, (PACK, LANES)).astype(BF16)
        for k, label in enumerate(labels):
            hit = jnp.where(wide == label, one, zero)
            total[k] = hit if total[k] is None else total[k] + hit
    return total


def lane_row(block):
    return jnp.concatenate([block[k : k + 1, :] for k in range(block.shape[0])], axis=1)


def shard_place():
    within = lax.axis_index("grp")
    return lax.axis_index("seq") * lax.axis_size("grp") + within, within


def first_kernel(rows, base, out_totals):
    devices = out_totals.shape[0]
    values = base[:rows, :]
    half = CODES // PACK
    labels = lax.broadcasted_iota(jnp.int32, (PACK, LANES), 0).astype(F32).astype(BF16)
    one, zero = jnp.ones((PACK, LANES), BF16), jnp.zeros((PACK, LANES), BF16)
    highs, lows = [], []
    for part, hits in (((values >> 4).astype(F32), highs), ((values & (half - 1)).astype(F32), lows)):
        for r in range(rows):
            wide = jnp.broadcast_to(part[r : r + 1, :], (PACK, LANES)).astype(BF16)
            hits.append(jnp.where(wide == labels, one, zero))
    pair = lax.dot_general(
        jnp.concatenate(highs, axis=1),
        jnp.concatenate(lows, axis=1),
        (((1,), (1,)), ((), ())),
        preferred_element_type=F32,
    )
    spread = jnp.concatenate([pair, jnp.zeros((PACK, LANES - half), F32)], axis=1)
    lines = []
    for k in range(CODES // LANES):
        step = LANES // half
        turn = pltpu.roll(spread[k * step : (k + 1) * step, :], 0, axis=1, stride=half, stride_axis=0)
        lines.append(jnp.sum(turn, axis=0, keepdims=True))
    total = jnp.concatenate(lines, axis=1)
    out_totals[...] = jnp.broadcast_to(total.reshape(1, 1, CODES), (devices, 1, CODES))


def block_tallies(left, source, count, labels):
    for g in range(count):
        found = tally_rows([source[g * BLOCK + i : g * BLOCK + i + 1, :] for i in range(BLOCK)], labels)
        for k, group in enumerate(found):
            left[k * PACK : (k + 1) * PACK, g * LANES : (g + 1) * LANES] = group


def block_kernel(rows, base, near, out_left, out_first, out_bounds, out_count, turned):
    shard = shard_place()[0]
    groups = LANES // BLOCK
    slots = out_bounds.shape[1]

    def used(ends):
        above = jnp.sum((ends > 0).astype(jnp.int32), axis=(0, 1), keepdims=True)
        return above + (ends[:1, :1] == 0).astype(jnp.int32)

    ends, prior_ends = base[rows:, :], near[rows:, :]
    out_bounds[:1, :] = lane_row(ends)
    wide = jnp.broadcast_to(lane_row(prior_ends), (8, slots))
    out_bounds[1:, :] = pltpu.roll(wide, slots - jnp.max(used(prior_ends)), axis=1)[:1, :]
    out_count[...] = jnp.broadcast_to(used(ends), (1, LANES))
    before = jnp.where(shard > 0, near[:rows, :], -1)
    turned[...] = jnp.concatenate([before, base[:rows, :]], axis=0).astype(F32).T
    block_tallies(out_left, turned, groups, label_groups())
    for g in range(groups):
        here = turned[g * BLOCK : (g + 1) * BLOCK, :]
        if g + 1 < groups:
            after = turned[(g + 1) * BLOCK : (g + 2) * BLOCK, :]
        else:
            after = pltpu.roll(turned[:BLOCK, :], LANES - 1, axis=1)
        out_left[CODES:, g * LANES : (g + 1) * LANES] = (after - here).astype(BF16)
    out_first[...] = turned[:BLOCK, :]


def main_kernel(left, first, bounds, count, handed, relayed, out_share, share_rows, out_run, out_weight,
                side, side_left, mask, parts, leave):
    shard, within = shard_place()
    tail_rows = relayed.shape[0] - 1
    tail = relayed.at[:tail_rows, :]
    slots = bounds.shape[1]
    rows = left.shape[1] * BLOCK // (2 * LANES)
    shard_len = rows * LANES
    out_rows = out_run.shape[0]
    groups = LANES // BLOCK
    side_blocks = side.shape[0] // BLOCK
    split = LANES // tail_rows
    labels = label_groups()

    far = jnp.where(shard > 1, tail[...], -1).astype(F32)
    step = LANES // split
    stacked = jnp.concatenate(
        [far] + [pltpu.roll(far, LANES - step * k, axis=1) for k in range(1, split)], axis=0
    )
    side[...] = stacked.T[:step, :]
    block_tallies(side_left, side, side_blocks, labels)
    lane = lax.broadcasted_iota(jnp.int32, (BLOCK, LANES), 1)
    for g in range(side_blocks):
        here = side[g * BLOCK : (g + 1) * BLOCK, :]
        if g + 1 < side_blocks:
            after = side[(g + 1) * BLOCK : (g + 2) * BLOCK, :]
        else:
            top = side[:BLOCK, :]
            after = jnp.where(
                lane < LANES - tail_rows,
                pltpu.roll(top, LANES - tail_rows, axis=1),
                pltpu.roll(top, LANES - tail_rows - 1, axis=1),
            )
            after = jnp.where(lane < LANES - 1, after, first[:, :1])
        side_left[CODES:, g * LANES : (g + 1) * LANES] = (after - here).astype(BF16)

    given = jnp.max(relayed[tail_rows:, :])
    arrived = jnp.where(within > 0, given, 0)
    kept = jnp.concatenate([count[...] - handed[...]] * (out_rows // LANES), axis=1)

    def moved(row, shift):
        return pltpu.roll(jnp.broadcast_to(row, (8, slots)), shift, axis=1)[:1, :out_rows]

    own = moved(bounds[:1, :], arrived)
    sent = moved(bounds[1:, :], given)
    row = lax.broadcasted_iota(jnp.int32, (1, out_rows), 1)
    end = jnp.where(row < arrived, sent - shard_len, own)
    valid = row < arrived + kept
    end = jnp.where(valid, end, 0)

    upper = end + 1 + shard_len
    lower = upper - WINDOW
    upper_block, lower_block = upper >> 4, lower >> 4
    down = lax.broadcasted_iota(jnp.int32, (PACK, out_rows), 0).astype(F32)
    downs = [(down + PACK * k).astype(BF16) for k in range(LANES // PACK)]
    one, zero = jnp.ones((PACK, out_rows), BF16), jnp.zeros((PACK, out_rows), BF16)

    def limit(value):
        bound = jnp.clip(value, 0, LANES).astype(F32)
        return jnp.broadcast_to(bound, (PACK, out_rows)).astype(BF16)

    for g in range(groups):
        high = limit((upper_block - g + groups - 1) >> 3)
        low = limit((lower_block - g + groups - 1) >> 3)
        for k in range(LANES // PACK):
            reach = jnp.where(downs[k] < high, one, zero)
            skip = jnp.where(downs[k] < low, one, zero)
            base = g * LANES + k * PACK
            mask[base : base + PACK, :out_rows] = reach - one if k * PACK < rows else reach
            mask[base : base + PACK, out_rows:] = reach - skip
    side_block = lower_block + tail_rows * groups
    for g in range(side_blocks):
        for part in range(split):
            low = limit((side_block - side_blocks * part - g + groups - 1) >> 3)
            for k in range(tail_rows // PACK):
                base = (groups + g) * LANES + part * tail_rows + k * PACK
                mask[base : base + PACK, out_rows:] = jnp.where(downs[k] < low, zero, one)

    main_depth = groups * LANES
    parts[:, :out_rows] = jnp.dot(
        left[...], mask[:main_depth, :out_rows], preferred_element_type=F32
    )
    parts[:, out_rows:] = jnp.dot(
        left[...], mask[:main_depth, out_rows:], preferred_element_type=F32
    ) + jnp.dot(side_left[...], mask[main_depth:, out_rows:], preferred_element_type=F32)

    upper_codes = parts[CODES:, :out_rows] + first[:, rows : rows + 1]
    lower_codes = upper_codes - parts[CODES:, out_rows:]
    inner = lax.broadcasted_iota(jnp.int32, (BLOCK, out_rows), 0)
    upper_codes = jnp.where(inner < (upper & (BLOCK - 1)), upper_codes, -2.0)
    lower_codes = jnp.where(inner < (lower & (BLOCK - 1)), lower_codes, -2.0)
    position = (shard * shard_len + end + 1).astype(F32)
    share_weight = jnp.where(valid, CODES / jnp.minimum(position, float(WINDOW)), 0.0)
    gap_weight = jnp.where(valid, CODES / position, 0.0)
    copies = []
    for q in range(out_rows // LANES):
        cut = slice(q * LANES, (q + 1) * LANES)
        ups = tally_rows([upper_codes[i : i + 1, cut] for i in range(BLOCK)], labels)
        lows = tally_rows([lower_codes[i : i + 1, cut] for i in range(BLOCK)], labels)
        lower_cut = slice(out_rows + q * LANES, out_rows + (q + 1) * LANES)
        shares, runs = [], []
        for k in range(CODES // PACK):
            span = slice(k * PACK, (k + 1) * PACK)
            up = ups[k].astype(F32)
            runs.append(parts[span, cut] + up)
            tally = parts[span, lower_cut] + (up - lows[k].astype(F32))
            shares.append(tally * share_weight[:, cut])
        share_rows[cut, :] = jnp.concatenate(shares, axis=0).T
        copies.append(pltpu.make_async_copy(share_rows.at[cut], out_share.at[cut], leave.at[q]))
        copies[-1].start()
        out_run[cut, :] = jnp.concatenate(runs, axis=0).T
        out_weight[cut, :] = jnp.broadcast_to(gap_weight[:, cut], (LANES, LANES)).T
    for copy in copies:
        copy.wait()


def last_kernel(totals, share, run, weight, out_gap, gap, sent):
    out_rows = share.shape[0]
    shard = shard_place()[0]
    offset = lax.fori_loop(0, shard, lambda j, before: before + totals[j], jnp.zeros((1, CODES), F32))
    pieces = out_rows // LANES
    copies = []
    for p in range(pieces):
        span = pl.ds(p * LANES, LANES)
        for k in range(CODES // LANES):
            cut = slice(k * LANES, (k + 1) * LANES)
            running = run[span, cut] + offset[:, cut]
            gap[span, cut] = share[span, cut] - running * weight[span, :]
        copies.append(pltpu.make_async_copy(gap.at[span], out_gap.at[span], sent.at[p]))
        copies[-1].start()
    for copy in copies:
        copy.wait()


def local(event_codes, window_ends, window_count, handed):
    group = lax.axis_size("grp")
    devices = lax.axis_size("seq") * group
    shard_len, slots = event_codes.shape[0], window_ends.shape[0]
    rows = shard_len // LANES
    tail_rows = WINDOW // LANES
    out_rows = 2 * slots // 3
    hbm = pl.BlockSpec(memory_space=pltpu.HBM)
    vmem = pl.BlockSpec(memory_space=pltpu.VMEM)
    params = pltpu.CompilerParams(vmem_limit_bytes=VMEM_LIMIT)
    to_next = [(i, (i + 1) % devices) for i in range(devices)]
    in_group = [(i, (i + 1) % group) for i in range(group)]

    base = jnp.concatenate(
        [event_codes.reshape(rows, LANES), window_ends.reshape(slots // LANES, LANES)]
    )
    near = lax.ppermute(base, AXES, to_next)
    totals = pl.pallas_call(
        functools.partial(first_kernel, rows),
        out_shape=jax.ShapeDtypeStruct((devices, 1, CODES), F32),
        in_specs=[vmem],
        out_specs=vmem,
        compiler_params=params,
        name="totals",
    )(base)
    everyone = lax.all_to_all(totals, AXES, 0, 0, tiled=True)
    passing = jnp.broadcast_to(handed[:, None], (1, LANES))
    packed = jnp.concatenate([near[rows - tail_rows : rows], passing])
    relayed = lax.ppermute(packed, "grp", in_group)

    depth = 2 * shard_len // BLOCK
    side_depth = WINDOW // BLOCK
    left, first, bounds, count = pl.pallas_call(
        functools.partial(block_kernel, rows),
        out_shape=(
            jax.ShapeDtypeStruct((CODES + BLOCK, depth), BF16),
            jax.ShapeDtypeStruct((BLOCK, LANES), F32),
            jax.ShapeDtypeStruct((2, slots), jnp.int32),
            jax.ShapeDtypeStruct((1, LANES), jnp.int32),
        ),
        in_specs=[vmem, vmem],
        out_specs=(vmem, vmem, vmem, vmem),
        scratch_shapes=[pltpu.VMEM((LANES, LANES), F32)],
        compiler_params=params,
        cost_estimate=pl.CostEstimate(
            flops=2 * CODES * depth * LANES, bytes_accessed=2**20, transcendentals=0
        ),
        name="blocks",
    )(base, near)
    share, near_share, run, weight = pl.pallas_call(
        main_kernel,
        out_shape=(
            jax.ShapeDtypeStruct((out_rows, CODES), F32),
            jax.ShapeDtypeStruct((out_rows, CODES), F32),
            jax.ShapeDtypeStruct((out_rows, CODES), F32),
            jax.ShapeDtypeStruct((out_rows, LANES), F32),
        ),
        in_specs=[vmem] * 6,
        out_specs=(hbm, vmem, vmem, vmem),
        scratch_shapes=[
            pltpu.VMEM((tail_rows, LANES), F32),
            pltpu.VMEM((CODES + BLOCK, side_depth), BF16),
            pltpu.VMEM((depth + side_depth, 2 * out_rows), BF16),
            pltpu.VMEM((CODES + BLOCK, 2 * out_rows), F32),
            pltpu.SemaphoreType.DMA((out_rows // LANES,)),
        ],
        compiler_params=params,
        cost_estimate=pl.CostEstimate(
            flops=2 * (CODES + BLOCK) * depth * 2 * out_rows,
            bytes_accessed=2**21,
            transcendentals=0,
        ),
        name="windows",
    )(left, first, bounds, count, passing, relayed)
    gap = pl.pallas_call(
        last_kernel,
        out_shape=jax.ShapeDtypeStruct((out_rows, CODES), F32),
        in_specs=[vmem] * 4,
        out_specs=hbm,
        scratch_shapes=[
            pltpu.VMEM((out_rows, CODES), F32),
            pltpu.SemaphoreType.DMA((out_rows // LANES,)),
        ],
        compiler_params=params,
        name="gap",
    )(everyone, near_share, run, weight)
    return share, gap


def solution(mesh):
    in_specs = (P(AXES), P(AXES), P(AXES), P(AXES))
    out_specs = (P(AXES, None), P(AXES, None))
    return jax.shard_map(local, mesh=mesh, in_specs=in_specs, out_specs=out_specs, check_vma=False)
```
